32 devices in a mesh: seq: 8 (over z, y), batch: 4 (over x, core).
Axes of the slice: x: 2, y: 2, z: 4, core: 2. Of those that a mesh axis runs over, the one named last changes fastest.
Arguments:
- tokens: bfloat16 [4, 8192, 1024], P('batch', 'seq'), may hold values from -6 to 6
- logits: bfloat16 [4, 8192, 256], P('batch', 'seq'), may hold values from -160 to 160
- slot_grad: bfloat16 [4, 256, 1024], P('batch', 'seq'), may hold values from -6 to 6
- phi_param: bfloat16 [1024, 256], P('seq'), may hold values from -0.1875 to 0.1875
Outputs:
- token_grad: bfloat16 [4, 8192, 1024], P('batch', 'seq')
- phi_grad: float32 [1024, 256], P('seq')
The draws below stay inside these ranges and needn't reach their ends.
All inputs are finite; a program needn't handle non-finite values.
Results may differ from the reference program's by a relative error of at most 0.0049.
Values may be sent and summed in bfloat16 or wider, within the bound.
No kernel may reach another device: no remote copies, remote signals or barrier semaphores. Data moves between devices by JAX's collectives and lax.ppermute only.
A program may use at most 64 MiB of HBM per device.

```python
import jax
import jax.numpy as jnp
from jax import lax

D = 1024
SLOTS = 256
TOK_DEV = 1024
SEQ_TOKENS = 8192
BATCH = 4


def draw_logits(key, part):
    key_base = jax.random.fold_in(key, 0)
    key_tilt = jax.random.fold_in(key, 1)
    key_offset = jax.random.fold_in(key, 3)
    block_count = SEQ_TOKENS // TOK_DEV
    values = jnp.clip(jax.random.normal(key_base, (BATCH, SEQ_TOKENS, SLOTS), jnp.float32), -6.0, 6.0) * 1.5
    block_tilt = jax.random.uniform(key_tilt, (BATCH, block_count, 1, SLOTS), jnp.float32, -2.0, 2.0)
    values = (values.reshape(BATCH, block_count, TOK_DEV, SLOTS) + block_tilt).reshape(BATCH, SEQ_TOKENS, SLOTS)
    offset = jax.random.uniform(key_offset, (SLOTS,), jnp.float32, -3.0, 3.0)
    values = values + offset
    return jnp.clip(values, -160.0, 160.0).astype(jnp.bfloat16)


def spiked(entries, key, source, target, parts, factor):
    def block_of(axis_at):
        return (jnp.arange(entries.shape[axis_at]) // (entries.shape[axis_at] // parts)).reshape((-1,) + (1,) * (entries.ndim - 1 - axis_at))

    one_side = jax.random.permutation(key, parts)[block_of(target)]
    other_side = (block_of(target) + parts // 2) % parts
    return jnp.where((block_of(source) == one_side) | (block_of(source) == other_side), factor * entries, entries)


def steps_of(rng, shape, shards, smallest, top_value):
    level = 1.0
    for position, parts in shards:
        steps = jax.random.uniform(jax.random.fold_in(jax.random.fold_in(rng, 6), position), (parts,), jnp.float32, smallest / len(shards), top_value / len(shards))
        level = level * jnp.repeat(jnp.exp(steps), shape[position] // parts).reshape((-1,) + (1,) * (len(shape) - 1 - position))
    return level


def scatter_about(rng, dims, spread, most, cuts=(), kind=jnp.bfloat16):
    drawn = spread * jax.random.normal(rng, dims, jnp.float32)
    if cuts:
        drawn = drawn * steps_of(rng, dims, cuts, -0.22, 0.18)
    return jnp.clip(drawn, -most, most).astype(kind)


def gaussian_with(rng, extent, deviation, bound, pieces, heavy, held_as=jnp.bfloat16):
    drawn = deviation * jax.random.normal(rng, extent, jnp.float32)
    if pieces:
        drawn = drawn * steps_of(rng, extent, pieces, -0.22, 0.18)
    return jnp.clip(spiked(drawn, jax.random.fold_in(rng, 3), *heavy), -bound, bound).astype(held_as)


def setup_inputs(seed: int = 0) -> dict:
    arg_keys = jax.random.split(jax.random.key(seed), 5)
    tokens = gaussian_with(arg_keys[0], (BATCH, SEQ_TOKENS, D), 1.0, 6.0, ((0, 4), (1, 8)), (1, 2, 8, 2.0))
    logits = draw_logits(jax.random.fold_in(arg_keys[4], 71), 0)
    slot_grad = scatter_about(arg_keys[2], (BATCH, SLOTS, D), 1.0, 6.0, ((0, 4), (1, 8)))
    phi_param = scatter_about(arg_keys[3], (D, SLOTS), D ** -0.5, 0.1875, ((0, 8),))
    return dict(tokens=tokens, logits=logits, slot_grad=slot_grad, phi_param=phi_param)


def reference(tokens, logits, slot_grad, phi_param):
    grad_scale = float(SEQ_TOKENS // 16)
    phi_grad = jnp.zeros((D, SLOTS), jnp.float32)
    results = []
    for seq_index in range(BATCH):
        inputs = tokens[seq_index]
        scores = logits[seq_index].astype(jnp.float32)
        upstream = slot_grad[seq_index]
        col_peak = jnp.max(scores, axis=0, keepdims=True)
        raw_weights = jnp.exp(scores - col_peak)
        col_total = jnp.sum(raw_weights, axis=0, keepdims=True)
        dispatch = raw_weights / col_total
        weight_grad = lax.dot_general(inputs, upstream, (((1,), (1,)), ((), ())), preferred_element_type=jnp.float32)
        col_dot = jnp.sum(dispatch * weight_grad, axis=0, keepdims=True)
        logit_grad = (dispatch * (weight_grad - col_dot)).astype(jnp.bfloat16)
        dispatch_low = dispatch.astype(jnp.bfloat16)
        token_sum = jnp.dot(dispatch_low, upstream, preferred_element_type=jnp.float32)
        token_sum = token_sum + lax.dot_general(logit_grad, phi_param, (((1,), (1,)), ((), ())), preferred_element_type=jnp.float32)
        results.append((grad_scale * token_sum).astype(jnp.bfloat16))
        phi_grad = phi_grad + lax.dot_general(inputs, logit_grad, (((0,), (0,)), ((), ())), preferred_element_type=jnp.float32)
    return jnp.stack(results), phi_grad
```

```python
import jax
import jax.numpy as jnp
from jax import lax
from jax.sharding import PartitionSpec as P


def spread(block, axis):
    count = lax.axis_size(axis)
    return lax.all_to_all(jnp.broadcast_to(block[None], (count,) + block.shape), axis, 0, 0)


def gathered(slot_part, phi_part):
    rows, width = slot_part.shape
    sharers = lax.axis_size("batch")
    if phi_part.size % (sharers * width):
        return spread(slot_part, "seq").reshape(-1, width), None
    piece = phi_part.reshape(sharers, -1, width)[lax.axis_index("batch")]
    both = spread(jnp.concatenate([slot_part, piece], axis=0), "seq")
    return both[:, :rows].reshape(-1, width), both[:, rows:]


def finished(phi_part, phi_pieces):
    slots = phi_part.shape[1]
    if phi_pieces is None:
        return spread(phi_part, "seq").reshape(-1, slots)
    pieces = lax.all_gather(phi_pieces, "batch", axis=0)
    return pieces.transpose(1, 0, 2, 3).reshape(-1, slots)


def per_device(tokens, logits, slot_grad, phi_param):
    inputs = tokens[0]
    scores = logits[0].astype(jnp.float32)
    upstream, phi_pieces = gathered(slot_grad[0], phi_param)
    width, slots = inputs.shape[1], scores.shape[1]
    part_peak = jnp.max(scores, axis=0, keepdims=True)
    raw_weights = jnp.exp(scores - part_peak)
    part_total = jnp.sum(raw_weights, axis=0, keepdims=True)
    weight_grad = lax.dot_general(
        inputs, upstream, (((1,), (1,)), ((), ())), preferred_element_type=jnp.float32
    )
    part_dot = jnp.sum(raw_weights * weight_grad, axis=0, keepdims=True)
    stats = spread(jnp.concatenate([part_peak, part_total, part_dot], axis=0), "seq")
    peaks, totals, dots = stats[:, 0], stats[:, 1], stats[:, 2]
    col_peak = jnp.max(peaks, axis=0, keepdims=True)
    rescale = jnp.exp(peaks - col_peak)
    col_total = jnp.sum(totals * rescale, axis=0, keepdims=True)
    col_dot = jnp.sum(dots * rescale, axis=0, keepdims=True) / col_total
    dispatch = raw_weights * (jnp.exp(part_peak - col_peak) / col_total)
    logit_grad = (dispatch * (weight_grad - col_dot)).astype(jnp.bfloat16)
    dispatch_low = dispatch.astype(jnp.bfloat16)
    phi_terms = lax.dot_general(
        inputs, logit_grad, (((0,), (0,)), ((), ())), preferred_element_type=jnp.float32
    ).astype(jnp.bfloat16)
    phi_terms, phi_pieces, phi_part = lax.optimization_barrier((phi_terms, phi_pieces, phi_param))
    owners = lax.axis_size(("seq", "batch"))
    phi_parts = lax.all_to_all(
        phi_terms.reshape(owners, width // owners, slots), ("seq", "batch"), 0, 0
    )
    phi_share = jnp.sum(phi_parts.astype(jnp.float32), axis=0)
    phi_grad = lax.all_gather(phi_share, "batch", axis=0, tiled=True)
    phi_full = finished(phi_part, phi_pieces)
    grad_scale = float(lax.axis_size("seq") * inputs.shape[0] // 16)
    token_sum = jnp.dot(dispatch_low, upstream, preferred_element_type=jnp.float32)
    token_sum = token_sum + lax.dot_general(
        logit_grad, phi_full, (((1,), (1,)), ((), ())), preferred_element_type=jnp.float32
    )
    token_grad = (grad_scale * token_sum).astype(jnp.bfloat16)[None]
    return (token_grad, phi_grad)


def solution(mesh):
    return jax.shard_map(
        per_device,
        mesh=mesh,
        in_specs=(
            P("batch", "seq", None),
            P("batch", "seq", None),
            P("batch", "seq", None),
            P("seq", None),
        ),
        out_specs=(P("batch", "seq", None), P("seq", None)),
        check_vma=False,
    )
```

```python
import jax
import jax.numpy as jnp
from jax import lax
from jax.sharding import PartitionSpec as P


def spread(block, axis):
    count = lax.axis_size(axis)
    return lax.all_to_all(jnp.broadcast_to(block[None], (count,) + block.shape), axis, 0, 0)


def crossed(block, axis, flip):
    count = lax.axis_size(axis)
    return lax.ppermute(block, axis, [(i, i ^ flip) for i in range(count)])


def collected(block, axis):
    count = lax.axis_size(axis)
    if count > 8 or count & (count - 1):
        return spread(block, axis)
    here = lax.axis_index(axis)
    half = count // 2
    far = crossed(block, axis, half)
    found = {0: block, half: far}
    for flip in range(1, half):
        found[flip] = crossed(block, axis, flip)
    for flip in range(1, half):
        found[half + flip] = crossed(far, axis, flip)
    out = jnp.zeros((count,) + block.shape, block.dtype)
    for flip, part in found.items():
        out = lax.dynamic_update_index_in_dim(out, part, here ^ flip, 0)
    return out


def gathered(slot_part, phi_part):
    rows, width = slot_part.shape
    sharers = lax.axis_size("batch")
    if phi_part.size % (sharers * width):
        return spread(slot_part, "seq").reshape(-1, width), None
    piece = phi_part.reshape(sharers, -1, width)[lax.axis_index("batch")]
    both = collected(jnp.concatenate([slot_part, piece], axis=0), "seq")
    return both[:, :rows].reshape(-1, width), both[:, rows:]


def finished(phi_part, phi_pieces):
    slots = phi_part.shape[1]
    if phi_pieces is None:
        return spread(phi_part, "seq").reshape(-1, slots)
    pieces = lax.all_gather(phi_pieces, "batch", axis=0)
    return pieces.transpose(1, 0, 2, 3).reshape(-1, slots)


def per_device(tokens, logits, slot_grad, phi_param):
    inputs = tokens[0]
    scores = logits[0].astype(jnp.float32)
    upstream, phi_pieces = gathered(slot_grad[0], phi_param)
    width, slots = inputs.shape[1], scores.shape[1]
    part_peak = jnp.max(scores, axis=0, keepdims=True)
    raw_weights = jnp.exp(scores - part_peak)
    part_total = jnp.sum(raw_weights, axis=0, keepdims=True)
    weight_grad = lax.dot_general(
        inputs, upstream, (((1,), (1,)), ((), ())), preferred_element_type=jnp.float32
    )
    part_dot = jnp.sum(raw_weights * weight_grad, axis=0, keepdims=True)
    stats = spread(jnp.concatenate([part_peak, part_total, part_dot], axis=0), "seq")
    peaks, totals, dots = stats[:, 0], stats[:, 1], stats[:, 2]
    col_peak = jnp.max(peaks, axis=0, keepdims=True)
    rescale = jnp.exp(peaks - col_peak)
    col_total = jnp.sum(totals * rescale, axis=0, keepdims=True)
    col_dot = jnp.sum(dots * rescale, axis=0, keepdims=True) / col_total
    dispatch = raw_weights * (jnp.exp(part_peak - col_peak) / col_total)
    logit_grad = (dispatch * (weight_grad - col_dot)).astype(jnp.bfloat16)
    dispatch_low = dispatch.astype(jnp.bfloat16)
    phi_terms = lax.dot_general(
        inputs, logit_grad, (((0,), (0,)), ((), ())), preferred_element_type=jnp.float32
    ).astype(jnp.bfloat16)
    phi_terms, phi_pieces, phi_part = lax.optimization_barrier((phi_terms, phi_pieces, phi_param))
    owners = lax.axis_size(("seq", "batch"))
    phi_parts = lax.all_to_all(
        phi_terms.reshape(owners, width // owners, slots), ("seq", "batch"), 0, 0
    )
    phi_share = jnp.sum(phi_parts.astype(jnp.float32), axis=0)
    phi_grad = lax.all_gather(phi_share, "batch", axis=0, tiled=True)
    phi_full = finished(phi_part, phi_pieces)
    grad_scale = float(lax.axis_size("seq") * inputs.shape[0] // 16)
    token_sum = jnp.dot(dispatch_low, upstream, preferred_element_type=jnp.float32)
    token_sum = token_sum + lax.dot_general(
        logit_grad, phi_full, (((1,), (1,)), ((), ())), preferred_element_type=jnp.float32
    )
    token_grad = (grad_scale * token_sum).astype(jnp.bfloat16)[None]
    return (token_grad, phi_grad)


def solution(mesh):
    return jax.shard_map(
        per_device,
        mesh=mesh,
        in_specs=(
            P("batch", "seq", None),
            P("batch", "seq", None),
            P("batch", "seq", None),
            P("seq", None),
        ),
        out_specs=(P("batch", "seq", None), P("seq", None)),
        check_vma=False,
    )
```

```python
import jax
import jax.numpy as jnp
from jax import lax
from jax.sharding import PartitionSpec as P


def spread(block, axis):
    count = lax.axis_size(axis)
    return lax.all_to_all(jnp.broadcast_to(block[None], (count,) + block.shape), axis, 0, 0)


def crossed(block, axis, flip):
    count = lax.axis_size(axis)
    return lax.ppermute(block, axis, [(i, i ^ flip) for i in range(count)])


def collected(block, axis):
    count = lax.axis_size(axis)
    if count > 8 or count & (count - 1):
        return spread(block, axis)
    here = lax.axis_index(axis)
    half = count // 2
    far = crossed(block, axis, half)
    found = {0: block, half: far}
    for flip in range(1, half):
        found[flip] = crossed(block, axis, flip)
    for flip in range(1, half):
        found[half + flip] = crossed(far, axis, flip)
    out = jnp.zeros((count,) + block.shape, block.dtype)
    for flip, part in found.items():
        out = lax.dynamic_update_index_in_dim(out, part, here ^ flip, 0)
    return out


def gathered(slot_part, phi_part):
    rows, width = slot_part.shape
    sharers = lax.axis_size("batch")
    if phi_part.size % (sharers * width) or width % phi_part.shape[1]:
        return spread(slot_part, "seq").reshape(-1, width), None
    piece = lax.dynamic_slice_in_dim(
        phi_part, lax.axis_index("batch") * (phi_part.shape[0] // sharers), phi_part.shape[0] // sharers, 0
    )
    piece = jnp.concatenate(jnp.split(piece, width // phi_part.shape[1], axis=0), axis=1)
    both = collected(jnp.concatenate([slot_part, piece], axis=0), "seq")
    return both[:, :rows].reshape(-1, width), both[:, rows:]


def finished(phi_part, phi_pieces):
    slots = phi_part.shape[1]
    if phi_pieces is None:
        return spread(phi_part, "seq").reshape(-1, slots)
    pieces = lax.all_gather(phi_pieces, "batch", axis=0)
    pieces = pieces.transpose(1, 0, 2, 3)
    columns = pieces.shape[3] // slots
    return jnp.stack(jnp.split(pieces, columns, axis=3), axis=2).reshape(-1, slots)


def per_device(tokens, logits, slot_grad, phi_param):
    inputs = tokens[0]
    scores = logits[0].astype(jnp.float32)
    upstream, phi_pieces = gathered(slot_grad[0], phi_param)
    width, slots = inputs.shape[1], scores.shape[1]
    part_peak = jnp.max(scores, axis=0, keepdims=True)
    raw_weights = jnp.exp(scores - part_peak)
    part_total = jnp.sum(raw_weights, axis=0, keepdims=True)
    weight_grad = lax.dot_general(
        inputs, upstream, (((1,), (1,)), ((), ())), preferred_element_type=jnp.float32
    )
    part_dot = jnp.sum(raw_weights * weight_grad, axis=0, keepdims=True)
    stats = spread(jnp.concatenate([part_peak, part_total, part_dot], axis=0), "seq")
    peaks, totals, dots = stats[:, 0], stats[:, 1], stats[:, 2]
    col_peak = jnp.max(peaks, axis=0, keepdims=True)
    rescale = jnp.exp(peaks - col_peak)
    col_total = jnp.sum(totals * rescale, axis=0, keepdims=True)
    col_dot = jnp.sum(dots * rescale, axis=0, keepdims=True) / col_total
    dispatch = raw_weights * (jnp.exp(part_peak - col_peak) / col_total)
    logit_grad = (dispatch * (weight_grad - col_dot)).astype(jnp.bfloat16)
    dispatch_low = dispatch.astype(jnp.bfloat16)
    phi_terms = lax.dot_general(
        inputs, logit_grad, (((0,), (0,)), ((), ())), preferred_element_type=jnp.float32
    ).astype(jnp.bfloat16)
    phi_terms, phi_pieces, phi_part = lax.optimization_barrier((phi_terms, phi_pieces, phi_param))
    owners = lax.axis_size(("seq", "batch"))
    phi_parts = lax.all_to_all(
        phi_terms.reshape(owners, width // owners, slots), ("seq", "batch"), 0, 0
    )
    phi_share = jnp.sum(phi_parts.astype(jnp.float32), axis=0)
    phi_grad = lax.all_gather(phi_share, "batch", axis=0, tiled=True)
    phi_full = finished(phi_part, phi_pieces)
    grad_scale = float(lax.axis_size("seq") * inputs.shape[0] // 16)
    token_sum = jnp.dot(dispatch_low, upstream, preferred_element_type=jnp.float32)
    token_sum = token_sum + lax.dot_general(
        logit_grad, phi_full, (((1,), (1,)), ((), ())), preferred_element_type=jnp.float32
    )
    token_grad = (grad_scale * token_sum).astype(jnp.bfloat16)[None]
    return (token_grad, phi_grad)


def solution(mesh):
    return jax.shard_map(
        per_device,
        mesh=mesh,
        in_specs=(
            P("batch", "seq", None),
            P("batch", "seq", None),
            P("batch", "seq", None),
            P("seq", None),
        ),
        out_specs=(P("batch", "seq", None), P("seq", None)),
        check_vma=False,
    )
```
